32 devices in a mesh: samp: 16 (over z, y, x), tgt: 2 (over core).
Axes of the slice: x: 2, y: 2, z: 4, core: 2. Of those that a mesh axis runs over, the one named last changes fastest.
Arguments:
- samples: bfloat16 [3072, 128], P('samp'), may hold values from -6 to 6
- omega: bfloat16 [128, 4096], replicated, may hold values from -0.5 to 0.5
- phase: float32 [4096], replicated, may hold values from -3.140625 to 3.140625
- right_side: float32 [4096, 512], P('samp', 'tgt'), may hold values from -6 to 6
Outputs:
- weights: float32 [4096, 512], P('samp', 'tgt')
The draws below stay inside these ranges and needn't reach their ends.
All inputs are finite; a program needn't handle non-finite values.
Results may differ from the reference program's by a relative error of at most 0.011.
The reference program's roundings to bfloat16 on the way count: a program that leaves them out, or rounds other values in their place, can miss the bound.
Values may be sent and summed in bfloat16 or wider, within the bound.
A program may use at most 128 MiB of HBM per device.

```python
import jax
import jax.numpy as jnp
from jax import lax

F = 4096
K = 512
DX = 128
ITERS = 2
N = 3072


def steps_of(rng, shape, shards, least, top_value):
    factor_of = 1.0
    for dim, blocks in shards:
        heights = jax.random.uniform(jax.random.fold_in(jax.random.fold_in(rng, 6), dim), (blocks,), jnp.float32, least / len(shards), top_value / len(shards))
        factor_of = factor_of * jnp.repeat(jnp.exp(heights), shape[dim] // blocks).reshape((-1,) + (1,) * (len(shape) - 1 - dim))
    return factor_of


def gaussian(rng, shape, deviation, bound, shards=(), held_as=jnp.bfloat16):
    values = jax.random.normal(rng, shape, jnp.float32) * deviation
    if len(shards) > 0:
        values = steps_of(rng, shape, shards, -0.22, 0.18) * values
    return jnp.clip(values, min=-bound, max=bound).astype(held_as)


def setup_inputs(seed: int = 0) -> dict:
    streams_of = jax.random.split(jax.random.key(seed), 5)
    return {
        "samples": gaussian(streams_of[0], (N, DX), 1.0, 6.0, ((0, 16),)),
        "omega": gaussian(streams_of[1], (DX, F), DX ** -0.5, 0.5),
        "phase": jnp.clip(jax.random.uniform(streams_of[2], (F,), jnp.float32, -3.140625, 3.140625), -3.140625, 3.140625),
        "right_side": gaussian(streams_of[3], (F, K), 1.0, 6.0, ((0, 16), (1, 2)), jnp.float32),
    }


ridge = 1.0

def precise_dot(left_matrix, right_matrix):
    return jnp.dot(left_matrix, right_matrix, precision=lax.Precision.HIGHEST)

def spd_solve(gram_matrix, rhs_matrix):
    factor = jnp.linalg.cholesky(gram_matrix)
    return jax.scipy.linalg.cho_solve((factor, True), rhs_matrix)

def reference(samples, omega, phase, right_side):
    preact = jnp.dot(samples.astype(jnp.float32), omega.astype(jnp.float32), preferred_element_type=jnp.float32) + phase
    features = jnp.cos(preact).astype(jnp.bfloat16)
    sample_total = features.shape[0]
    weights = jnp.zeros_like(right_side)
    residual = right_side
    direction = right_side
    gram_rr = precise_dot(residual.T, residual)
    for iteration in range(ITERS):
        projected = jnp.dot(features.astype(jnp.float32), direction.astype(jnp.bfloat16).astype(jnp.float32), preferred_element_type=jnp.float32).astype(jnp.bfloat16)
        image = jnp.dot(features.T.astype(jnp.float32), projected.astype(jnp.float32), preferred_element_type=jnp.float32) / sample_total + ridge * direction
        alpha_coef = spd_solve(precise_dot(direction.T, image), gram_rr)
        weights = weights + precise_dot(direction, alpha_coef)
        residual = residual - precise_dot(image, alpha_coef)
        gram_new = precise_dot(residual.T, residual)
        beta_coef = spd_solve(gram_rr, gram_new)
        direction = residual + precise_dot(direction, beta_coef)
        gram_rr = gram_new
    return weights
```

```python
import jax
import jax.numpy as jnp
from jax import lax
from jax.experimental import pallas as pl
from jax.experimental.pallas import tpu as pltpu
from jax.sharding import PartitionSpec as P

ridge = 1.0
HI = lax.Precision.HIGHEST
F32 = jnp.float32
BF16 = jnp.bfloat16
BLOCK = 128
GROUP = 4


def precise_dot(left_matrix, right_matrix):
    return jnp.dot(left_matrix, right_matrix, precision=HI, preferred_element_type=F32)


def gram_dot(left_matrix, right_matrix):
    return lax.dot_general(
        left_matrix, right_matrix, (((0,), (0,)), ((), ())), precision=HI, preferred_element_type=F32
    )


def cosine(x):
    n = jnp.round(x * 0.3183098861837907)
    r = x - n * 3.140625
    r = r - n * 9.67025756835938e-4
    r = r - n * 6.2771141529083251953e-7
    half = n * 0.5
    sign = 1.0 - 4.0 * (half - jnp.floor(half))
    s = r * r
    p = 2.08767569878681e-9
    for coef in (
        -2.755731922398589e-7,
        2.48015873015873e-5,
        -1.388888888888889e-3,
        4.166666666666667e-2,
        -0.5,
        1.0,
    ):
        p = p * s + coef
    return p * sign


def invert_small(pivots):
    size = len(pivots)
    held = [list(line) for line in pivots]
    for j in range(size):
        inverse = 1.0 / held[j][j]
        line = [inverse if m == j else held[j][m] * inverse for m in range(size)]
        for i in range(size):
            if i != j:
                factor = held[i][j]
                held[i] = [
                    -factor * line[m] if m == j else held[i][m] - factor * line[m] for m in range(size)
                ]
        held[j] = line
    return held


def invert_blocks(values):
    size = values[0].shape[0]
    many = [[value[t * 8 : t * 8 + 8, :] for t in range(size // 8)] for value in values]
    lane = lax.broadcasted_iota(jnp.int32, (8, size), 1)
    sub = lax.broadcasted_iota(jnp.int32, (8, size), 0)
    for j in range(0, size, GROUP):
        home, inner = divmod(j, 8)
        in_group = (lane >= j) & (lane < j + GROUP)
        for which, tiles in enumerate(many):
            rows = [
                jnp.broadcast_to(tiles[home][inner + k : inner + k + 1, :], (8, size)) for k in range(GROUP)
            ]
            pivots = invert_small(
                [[jnp.broadcast_to(row[:, j + m : j + m + 1], (8, size)) for m in range(GROUP)] for row in rows]
            )
            scaled = []
            for k in range(GROUP):
                line = pivots[k][0] * rows[0]
                for m in range(1, GROUP):
                    line = line + pivots[k][m] * rows[m]
                for m in range(GROUP):
                    line = jnp.where(lane == j + m, pivots[k][m], line)
                scaled.append(line)
            nxt = []
            for t, tile in enumerate(tiles):
                new = jnp.where(in_group, 0.0, tile)
                for k in range(GROUP):
                    new = new - jnp.broadcast_to(tile[:, j + k : j + k + 1], (8, size)) * scaled[k]
                if t == home:
                    for k in range(GROUP):
                        new = jnp.where(sub == inner + k, scaled[k], new)
                nxt.append(new)
            many[which] = nxt
    return [jnp.concatenate(tiles, axis=0) for tiles in many]


def spd_kernel(gram_ref, rhs_ref, out_ref, work):
    systems, total = gram_ref.shape[:2]
    size = BLOCK
    work[...] = gram_ref[...]
    out_ref[...] = rhs_ref[...]

    def step(k, carry):
        at = pl.ds(pl.multiple_of(k * size, size), size)
        inverses = invert_blocks([work[s, at, at] for s in range(systems)])
        for s in range(systems):
            inv = inverses[s]
            row_a = precise_dot(inv, work[s, at, :])
            row_x = precise_dot(inv, out_ref[s, at, :])
            for i in range(total // size):
                rows = pl.ds(i * size, size)
                left = jnp.where(k == i, 0.0, work[s, rows, at])
                work[s, rows, :] = work[s, rows, :] - precise_dot(left, row_a)
                out_ref[s, rows, :] = out_ref[s, rows, :] - precise_dot(left, row_x)
            work[s, at, :] = row_a
            out_ref[s, at, :] = row_x
        return carry

    lax.fori_loop(0, total // size, step, 0)


def spd_solve(gram_matrices, rhs_matrices):
    systems, total, cols = rhs_matrices.shape
    return pl.pallas_call(
        spd_kernel,
        out_shape=jax.ShapeDtypeStruct((systems, total, cols), F32),
        in_specs=[pl.BlockSpec(memory_space=pltpu.VMEM)] * 2,
        out_specs=pl.BlockSpec(memory_space=pltpu.VMEM),
        scratch_shapes=[pltpu.VMEM((systems, total, total), F32)],
        compiler_params=pltpu.CompilerParams(vmem_limit_bytes=24 * 2**20),
        cost_estimate=pl.CostEstimate(flops=2 * 10**10, bytes_accessed=3 * 2**20, transcendentals=0),
        name="spd",
    )(gram_matrices, rhs_matrices)


def full_gram(piece):
    summed = lax.psum(piece, "samp")
    return lax.all_gather(summed, "tgt", axis=1, tiled=True)


def body(samples, omega, phase, right_side):
    col_count = right_side.shape[1]
    sample_total = samples.shape[0] * lax.axis_size("samp")
    col_offset = lax.axis_index("tgt") * col_count

    def own(matrix):
        return lax.dynamic_slice_in_dim(matrix, col_offset, col_count, 1)

    def wide(matrix):
        return lax.all_gather(matrix, "tgt", axis=1, tiled=True)

    right_cols = lax.all_gather(right_side.astype(BF16), "samp", axis=0, tiled=True)
    right_all = wide(right_side)
    gram_rr = full_gram(gram_dot(right_all, right_side))
    feats = cosine(jnp.dot(samples, omega, preferred_element_type=F32) + phase).astype(BF16)

    projected = jnp.dot(feats, right_cols, preferred_element_type=F32).astype(BF16)
    lifted = lax.dot_general(feats, projected, (((0,), (0,)), ((), ())), preferred_element_type=F32)
    lifted_own = lax.psum_scatter(lifted, "samp", scatter_dimension=0, tiled=True) / sample_total
    proj_all = wide(projected)
    gram_py = full_gram(
        lax.dot_general(proj_all, projected, (((0,), (0,)), ((), ())), preferred_element_type=F32)
    )
    gram_pq = gram_py / sample_total + ridge * gram_rr
    unit = jnp.eye(gram_rr.shape[0], dtype=F32)
    solved = spd_solve(jnp.stack([gram_pq, gram_rr]), jnp.stack([gram_rr, unit]))
    alpha, gram_inverse = solved[0], solved[1]

    lifted_all = wide(lifted_own)
    resid_all = right_all - precise_dot(lifted_all + ridge * right_all, alpha)
    resid_own = own(resid_all)
    resid_cols = lax.all_gather(resid_own.astype(BF16), "samp", axis=0, tiled=True)
    gram_new = full_gram(gram_dot(resid_all, resid_own))
    beta = precise_dot(gram_inverse, gram_new)
    direction_all = resid_all + precise_dot(right_all, beta)
    carried = precise_dot(proj_all.astype(F32), own(beta))

    second = (jnp.dot(feats, resid_cols, preferred_element_type=F32) + carried).astype(BF16)
    gram_two = full_gram(
        lax.dot_general(wide(second), second, (((0,), (0,)), ((), ())), preferred_element_type=F32)
        / sample_total
        + ridge * gram_dot(direction_all, own(direction_all))
    )
    alpha_two = spd_solve(gram_two[None], own(gram_new)[None])[0]
    return precise_dot(right_all, own(alpha)) + precise_dot(direction_all, alpha_two)


def solution(mesh):
    placed = (P("samp", None), P(), P(), P("samp", "tgt"))
    return jax.shard_map(
        body, mesh=mesh, in_specs=placed, out_specs=P("samp", "tgt"), check_vma=False
    )
```
